128 devices in a mesh: dp: 2 (over x_lo), expert: 32 (over y, z, core), tensor: 2 (over x_hi).
Axes of the slice: x: 4 (x_hi: 2, x_lo: 2; x = x_hi * 2 + x_lo), y: 4, z: 4, core: 2. Of those that a mesh axis runs over, the one named last changes fastest.
Arguments:
- tokens: bfloat16 [8192, 2048], P(('dp', 'expert')), may hold values from -6 to 6
- norm_gain: float32 [2048], replicated, may hold values from 0.1 to 1.9
- router: bfloat16 [2048, 32], replicated, may hold values from -0.125 to 0.125
- expert_ids: int32 [8192, 4], P(('dp', 'expert')), may hold values from 0 to 31, all different within a row; in each aligned block of 128 rows (0 to 127, 128 to 255, ...) at most 20 rows name the same one
- modality: int32 [8192], P(('dp', 'expert')), may hold values from 0 to 1, as said below
- expert_gate: bfloat16 [32, 2048, 1408], P('expert', None, 'tensor'), may hold values from -0.125 to 0.125
- expert_up: bfloat16 [32, 2048, 1408], P('expert', None, 'tensor'), may hold values from -0.125 to 0.125
- expert_down: bfloat16 [32, 1408, 2048], P('expert', 'tensor'), may hold values from -0.15625 to 0.15625
- shared_gate: bfloat16 [2, 2048, 704], P(None, None, ('dp', 'tensor')), may hold values from -0.125 to 0.125
- shared_up: bfloat16 [2, 2048, 704], P(None, None, ('dp', 'tensor')), may hold values from -0.125 to 0.125
- shared_down: bfloat16 [2, 704, 2048], P(None, ('dp', 'tensor')), may hold values from -0.21875 to 0.21875
Outputs:
- mixed: bfloat16 [8192, 2048], P(('dp', 'expert'), 'tensor')
The draws below stay inside these ranges and needn't reach their ends.
Inputs may be any that keep to these rules, and one draw needn't show every extreme that they name: `expert_ids`: each token names 4 different experts; among the 128 tokens of one device (aligned blocks of rows) no expert is named by more than 20 tokens, and some expert reaches 20. `modality`: within each aligned block of 128 tokens the image patches form one run (taken cyclically) that covers from an eighth to seven eighths of the block.
All inputs are finite; a program needn't handle non-finite values.
Results may differ from the reference program's by a relative error of at most 0.0073.
Values may be sent and summed in bfloat16 or wider, within the bound.
A program may use at most 128 MiB of HBM per device.

```python
import math
import jax
import jax.numpy as jnp
import numpy as np
from jax import lax

D = 2048
FF = 1408
SH = 704
TOP = 4
TOK_DEV = 128
EXPERTS = 32
TOKENS = 8192
CAP = 20


def draw_modality(key, part):
    blocks = TOKENS // TOK_DEV
    share_key, start_key = jax.random.split(jax.random.fold_in(key, 11))
    counts = jax.random.randint(share_key, (blocks, 1), TOK_DEV // 8, TOK_DEV - TOK_DEV // 8 + 1)
    starts = jax.random.randint(start_key, (blocks, 1), 0, TOK_DEV)
    position = jnp.arange(TOK_DEV, dtype=jnp.int32)[None, :]
    image_flags = ((position - starts) % TOK_DEV < counts).astype(jnp.int32)
    return image_flags.reshape(-1)


def steps_of(stream_key, shape, pieces, smallest, high):
    loudness, own = 1.0, jax.random.fold_in(stream_key, 6)
    for dim, blocks in pieces:
        draws = jnp.exp(jax.random.uniform(jax.random.fold_in(own, dim), (blocks,), jnp.float32, smallest / len(pieces), high / len(pieces)))
        loudness = loudness * jnp.repeat(draws, shape[dim] // blocks).reshape([-1 if axis == dim else 1 for axis in range(len(shape))])
    return loudness


def deal_out(rng, own, number, rows, amount, top, bound, slope):
    ranking = jax.random.permutation(rng, amount)
    heavy_load, usual = portions_of(amount, rows * top, bound, slope, True), portions_of(amount, rows * top, bound, slope, False)
    places = jnp.arange(amount)

    def named(tallies, rotation):
        used = int((tallies > 0).sum())
        fixed = max(1, used // 4)
        passed = fixed + (places - fixed + rotation * (used - fixed)) % max(1, amount - fixed)
        return jnp.zeros((amount,), jnp.int32).at[ranking[jnp.where(places < fixed, places, passed)]].set(jnp.asarray(tallies, jnp.int32))

    tallies = jnp.where(number % 4 == 0, named(heavy_load, number // 4), named(usual, number - number // 4 - 1))
    mixed = jax.random.permutation(jax.random.fold_in(own, 3), amount)
    giver, sink = mixed[0:amount // 2 * 2:2], mixed[1:amount // 2 * 2:2]
    margin = jnp.minimum(tallies[giver] - 1, bound - tallies[sink]) // 2
    margin = jnp.where((giver == ranking[0]) | (sink == ranking[0]) | (tallies[sink] == 0), 0, jnp.maximum(margin, 0))
    passed = jax.random.randint(jax.random.fold_in(own, 4), (amount // 2,), 0, 1 << 20) % (margin + 1)
    tallies = tallies.at[giver].add(-passed).at[sink].add(passed)
    labels = jnp.searchsorted(jnp.cumsum(tallies), jnp.arange(rows * top), side="right").astype(jnp.int32)
    listing = labels.reshape(top, rows).T
    listing = listing[jax.random.permutation(jax.random.fold_in(own, 1), rows)]
    rotation = jax.random.randint(jax.random.fold_in(own, 2), (rows, 1), 0, top)
    return jnp.take_along_axis(listing, (jnp.arange(top)[None, :] + rotation) % top, axis=1)


def portions_of(amount, total, reach, skew, full):
    weights = [(1 << 20) // math.isqrt(rank ** skew) + 1 for rank in range(1, amount + 1)]
    largest = reach if full else min(reach, max(-(-total // amount), total * weights[0] // sum(weights)))
    least = 1 if total - largest >= amount - 1 else 0
    given, spare = [largest] + [least] * (amount - 1), total - largest - least * (amount - 1)
    while spare > 0:
        free = [i for i in range(1, amount) if given[i] < largest] or [i for i in range(1, amount) if given[i] < reach]
        whole, left = sum([weights[i] for i in free]), spare
        for i in free:
            addition = min(reach - given[i], max(1, left * weights[i] // whole), spare)
            given[i] = given[i] + addition
            spare = spare - addition
    return np.array(given)


def bell_draw(rng, dims, scale, limit, pieces=(), held_as=jnp.bfloat16):
    array = scale * jax.random.normal(rng, dims, jnp.float32)
    if pieces:
        array = array * steps_of(rng, dims, pieces, -0.22, 0.18)
    return jnp.clip(array, -limit, limit).astype(held_as)


def setup_inputs(seed: int = 0) -> dict:
    key_list = jax.random.split(jax.random.key(seed), 12)
    tokens = bell_draw(key_list[0], (TOKENS, D), 1.0, 6.0, ((0, 64),))
    norm_gain = jnp.clip(1.0 + 0.18 * jax.random.normal(key_list[1], (D,), jnp.float32), 0.1, 1.9)
    router = bell_draw(key_list[2], (D, EXPERTS), D ** -0.5, 0.125)
    expert_ids_keys = jax.random.split(jax.random.fold_in(key_list[3], 1), TOKENS // TOK_DEV)
    expert_ids_turns = jax.random.permutation(jax.random.fold_in(key_list[3], 3), TOKENS // TOK_DEV)
    expert_ids = jax.vmap(lambda own, number: deal_out(jax.random.fold_in(key_list[3], 2), own, number, TOK_DEV, EXPERTS, TOP, CAP, 1))(expert_ids_keys, expert_ids_turns).reshape((TOKENS, TOP))
    modality = draw_modality(jax.random.fold_in(key_list[11], 71), 0)
    expert_gate = bell_draw(key_list[5], (EXPERTS, D, FF), D ** -0.5, 0.125, ((0, 32), (2, 2)))
    expert_up = bell_draw(key_list[6], (EXPERTS, D, FF), D ** -0.5, 0.125, ((0, 32), (2, 2)))
    expert_down = bell_draw(key_list[7], (EXPERTS, FF, D), FF ** -0.5, 0.15625, ((0, 32), (1, 2)))
    shared_gate = bell_draw(key_list[8], (2, D, SH), D ** -0.5, 0.125, ((2, 4),))
    shared_up = bell_draw(key_list[9], (2, D, SH), D ** -0.5, 0.125, ((2, 4),))
    shared_down = bell_draw(key_list[10], (2, SH, D), SH ** -0.5, 0.21875, ((1, 4),))
    return {"tokens": tokens, "norm_gain": norm_gain, "router": router, "expert_ids": expert_ids, "modality": modality, "expert_gate": expert_gate, "expert_up": expert_up, "expert_down": expert_down, "shared_gate": shared_gate, "shared_up": shared_up, "shared_down": shared_down}


epsilon = 1e-06

def rms_normed(tokens, norm_gain):
    values = tokens.astype(jnp.float32)
    inv_scale = lax.rsqrt(lax.optimization_barrier(jnp.mean(values * values, axis=-1, keepdims=True)) + epsilon)
    return (values * inv_scale * norm_gain).astype(jnp.bfloat16)

def route_weights(normed, router, expert_ids):
    logits = jnp.dot(normed, router, preferred_element_type=jnp.float32)
    chosen = jnp.take_along_axis(logits, expert_ids, axis=1)
    scores = jax.nn.sigmoid(chosen)
    return scores / lax.optimization_barrier(jnp.sum(scores, axis=1, keepdims=True))

def capacity_slots(expert_ids, expert_count, block_rows):
    row_count, top_count = expert_ids.shape
    onehot = (expert_ids[:, :, None] == jnp.arange(expert_count, dtype=jnp.int32)[None, None, :]).astype(jnp.int32)
    grouped = onehot.reshape(row_count // block_rows, block_rows * top_count, expert_count)
    running = (jnp.cumsum(grouped, axis=1, dtype=jnp.int32) - 1).reshape(row_count, top_count, expert_count)
    return lax.optimization_barrier(jnp.sum(running * onehot, axis=-1, dtype=jnp.int32)).astype(jnp.int32)

def reference(tokens, norm_gain, router, expert_ids, modality, expert_gate, expert_up, expert_down, shared_gate, shared_up, shared_down):
    normed = rms_normed(tokens, norm_gain)
    weights = route_weights(normed, router, expert_ids)
    slot_rank = capacity_slots(expert_ids, EXPERTS, TOK_DEV)
    sources = TOKENS // TOK_DEV
    token_index = jnp.broadcast_to(jnp.arange(TOKENS, dtype=jnp.int32)[:, None], (TOKENS, TOP)).astype(jnp.int32)
    source_block = (token_index // TOK_DEV).astype(jnp.int32)
    slot_table = jnp.full((EXPERTS, sources, CAP), TOKENS, jnp.int32)
    slot_table = slot_table.at[expert_ids, source_block, slot_rank].set(token_index)
    weight_table = jnp.zeros((EXPERTS, sources, CAP), jnp.float32)
    weight_table = weight_table.at[expert_ids, source_block, slot_rank].set(weights)
    padded = jnp.concatenate([normed, jnp.zeros((1, D), jnp.bfloat16)], axis=0)

    def one_expert(routed, operands):
        rows_index, slot_weight, gate_weight, up_weight, down_weight = operands
        flat_index = rows_index.reshape(-1)
        gathered = padded[flat_index]
        gate_value = jnp.dot(gathered, gate_weight, preferred_element_type=jnp.float32)
        up_value = jnp.dot(gathered, up_weight, preferred_element_type=jnp.float32)
        hidden = (jax.nn.silu(gate_value) * up_value).astype(jnp.bfloat16)
        result = jnp.dot(hidden, down_weight, preferred_element_type=jnp.float32)
        result = result * slot_weight.reshape(-1)[:, None]
        return (routed.at[flat_index].add(result), None)
    start = jnp.zeros((TOKENS + 1, D), jnp.float32)
    routed, unused = lax.scan(one_expert, start, (slot_table, weight_table, expert_gate, expert_up, expert_down))
    routed = routed[:TOKENS]

    def shared_out(modal_index):
        gate_value = jnp.dot(normed, shared_gate[modal_index], preferred_element_type=jnp.float32)
        up_value = jnp.dot(normed, shared_up[modal_index], preferred_element_type=jnp.float32)
        hidden = (jax.nn.silu(gate_value) * up_value).astype(jnp.bfloat16)
        return jnp.dot(hidden, shared_down[modal_index], preferred_element_type=jnp.float32)
    is_image = (modality == 1)[:, None]
    shared = jnp.where(is_image, shared_out(0), shared_out(1))
    return (shared + routed).astype(jnp.bfloat16)
```

```python
import jax
import jax.numpy as jnp
from jax import lax
from jax.experimental import pallas as pl
from jax.experimental.pallas import tpu as pltpu
from jax.sharding import PartitionSpec as P

MESH = pl.DeviceIdType.MESH
F32, BF16 = jnp.float32, jnp.bfloat16
RING = 4
EPS = 1e-06
UNPICKED = -100.0
ORDER = (0, 1, 3, 2)


def dot(a, b):
    return lax.dot_general(a, b, (((1,), (0,)), ((), ())), preferred_element_type=F32)


def silu(v):
    return v / (1.0 + jnp.exp(-v))


def kernel(
    tokens, gain, router, ids, flags, gate_h, up_h, down_h, sgate_h, sup_h, sdown_h, out,
    gate, up, down, sgate, sup, sdown,
    ag, meta, sel, place, weigh, slots, recv, gacc, uacc, hid, yout, back, rs_out, rs_in,
    x_out, x_in, sown, soth, sh_in, xfer_out, xfer_in, own,
    w_sem, g_s, g_r, m_s, m_r, xs_s, xs_r, d_s, d_r, b_s, b_r, r_s, r_r, sh_s, sh_r, t_s, t_r,
):
    rows, width = tokens.shape
    half = width // 2
    cap = recv.shape[0] // 32
    slab = RING * cap
    dp, me, tp = lax.axis_index("dp"), lax.axis_index("expert"), lax.axis_index("tensor")
    y, z, c = me // 8, (me % 8) // 2, me % 2
    dpo, tpo = 1 - dp, 1 - tp

    def at(yy, zz, cc):
        return (dp, yy * 8 + zz * 2 + cc, tp)

    def along_y(k):
        return (y + k) % RING

    def along_z(k):
        return (z + k) % RING

    def ring1(k):
        return at(c * along_y(k) + (1 - c) * y, (1 - c) * along_z(k) + c * z, c)

    def expert_of(k, cc):
        return (c * y + (1 - c) * along_y(k)) * 8 + (c * along_z(k) + (1 - c) * z) * 2 + cc

    def ring2(k, cc):
        return (dp, expert_of(k, cc), tp)

    def source(k, cs):
        return at(along_y(RING - k), z, 0) if cs == 0 else at(y, along_z(RING - k), 1)

    def mult(v, m):
        return pl.multiple_of(v, m)

    loads = [
        pltpu.make_async_copy(s, d, w_sem.at[i])
        for i, (s, d) in enumerate(
            [(sgate_h, sgate), (sup_h, sup), (sdown_h, sdown), (gate_h.at[0], gate), (up_h.at[0], up), (down_h.at[0], down)]
        )
    ]
    for cp in loads:
        cp.start()

    barrier = pltpu.get_barrier_semaphore()
    peers = [at(y, z, 1 - c), (dpo, me, 0), (dpo, me, 1), (dp, me, tpo)]
    for k in range(1, RING):
        for cc in range(2):
            peers += [at(along_y(k), z, cc), at(y, along_z(k), cc)]
    for peer in peers:
        pl.semaphore_signal(barrier, inc=1, device_id=peer, device_id_type=MESH)

    def remote(src, dst, ssem, rsem, dev):
        return pltpu.make_async_remote_copy(
            src_ref=src, dst_ref=dst, send_sem=ssem, recv_sem=rsem, device_id=dev, device_id_type=MESH
        )

    step = 32

    def norm_rows(i, carry):
        at_rows = pl.ds(mult(i * step, step), step)
        v = tokens[at_rows, :].astype(F32)
        inv = lax.rsqrt(jnp.mean(v * v, axis=-1, keepdims=True) + EPS)
        ag[at_rows, :] = (v * inv * gain[...]).astype(BF16)
        return carry

    lax.fori_loop(0, rows // step, norm_rows, 0)
    pl.semaphore_wait(barrier, len(peers))

    def cols(h):
        return pl.ds(h * half, half)

    def gather(h, j):
        return remote(
            ag.at[pl.ds(0, rows), cols(h)], ag.at[pl.ds(j * rows, rows), cols(h)], g_s.at[h, j], g_r.at[h, j], ring1(j)
        )

    for j in (2, 1, 3):
        gather(0, j).start()

    mine = pl.ds(mult(tp * half, half), half)
    theirs = pl.ds(mult(tpo * half, half), half)
    flag_rows = jnp.transpose(jnp.broadcast_to(flags[...].astype(F32), (rows, rows)))
    x_out[:, pl.ds(0, half)] = ag[pl.ds(0, rows), mine]
    x_out[:, pl.ds(half, 128)] = flag_rows.astype(BF16)

    def dp_rows(t):
        return remote(x_out, x_in.at[tp], xs_s.at[t], xs_r.at[tp], (dpo, me, t))

    def dp_rows_in(t):
        return remote(x_out, x_in.at[t], xs_s.at[t], xs_r.at[t], (dpo, me, t))

    for t in range(2):
        dp_rows(t).start()

    lane = lax.broadcasted_iota(jnp.int32, (rows, 128), 1)
    sub = lax.broadcasted_iota(jnp.int32, (rows, 128), 0)
    chosen = jnp.zeros((rows, 128), F32)
    for k in range(ids.shape[1]):
        chosen = chosen + (ids[:, k : k + 1] == lane).astype(F32)
    earlier = (lane < sub).astype(BF16)
    rank = dot(earlier, chosen.astype(BF16))
    logits = dot(ag[pl.ds(0, rows), :], router[...])
    score = chosen[:, :32] / (1.0 + jnp.exp(-logits))
    weight = score / jnp.sum(score, axis=1, keepdims=True)
    shift = (
        lax.broadcasted_iota(jnp.int32, (32, 128), 1) == lax.broadcasted_iota(jnp.int32, (32, 128), 0) + 32
    ).astype(BF16)
    moved = dot(weight.astype(BF16), shift)
    ranked = jnp.where(chosen > 0.0, rank, UNPICKED)
    meta[pl.ds(0, rows), :] = jnp.where(lane < 32, ranked, moved).astype(BF16)

    def meta_copy(j):
        return remote(meta.at[pl.ds(0, rows)], meta.at[pl.ds(j * rows, rows)], m_s.at[j], m_r.at[j], ring1(j))

    for j in (2, 1, 3):
        meta_copy(j).start()
    for j in (2, 1, 3):
        gather(1, j).start()

    for cp in loads[:3]:
        cp.wait()

    def shared(read_rows, keep, write):
        hidden = []
        for m in range(2):
            g = jnp.zeros((rows, sgate.shape[2]), F32)
            u = jnp.zeros((rows, sgate.shape[2]), F32)
            for h in range(2):
                part = read_rows(h)
                g = g + dot(part, sgate[m, cols(h), :])
                u = u + dot(part, sup[m, cols(h), :])
            picked = keep if m == 0 else 1.0 - keep
            hidden.append((silu(g) * u * picked).astype(BF16))
        for h in range(2):
            write(h, dot(hidden[0], sdown[0, :, cols(h)]) + dot(hidden[1], sdown[1, :, cols(h)]))

    def write_own(h, v):
        sown[:, cols(h)] = v

    shared(lambda h: ag[pl.ds(0, rows), cols(h)], flag_rows[:, :1], write_own)

    for s in range(8):
        e = expert_of(s // 2, s % 2)
        sel[pl.ds(s * slab, slab), :] = (lax.broadcasted_iota(jnp.int32, (slab, 128), 1) == e).astype(BF16)
    for j in (2, 1, 3):
        meta_copy(j).wait_recv()
    slot_row = lax.broadcasted_iota(jnp.int32, (slab, rows), 0).astype(F32)
    col = lax.broadcasted_iota(jnp.int32, (1, 8 * slab), 1)
    e_col = jnp.zeros((1, 8 * slab), jnp.int32)
    r_col = col
    for s in range(8):
        inside = (col >= s * slab) & (col < (s + 1) * slab)
        e_col = jnp.where(inside, expert_of(s // 2, s % 2), e_col)
        r_col = jnp.where(inside, col - s * slab, r_col)
    r_col = r_col.astype(F32)
    wide = lax.broadcasted_iota(jnp.int32, (128, 8 * slab), 0)
    sel_pos = (wide == e_col).astype(BF16)
    sel_w = (wide == e_col + 32).astype(BF16)
    for j in range(RING):
        block = meta[pl.ds(j * rows, rows), :]
        turned = jnp.transpose(block.astype(F32)).astype(BF16)
        turned_pos = dot(sel[...], turned)
        for s in range(8):
            part = turned_pos[s * slab : (s + 1) * slab, :]
            place[pl.ds(s * slab, slab), pl.ds(j * rows, rows)] = jnp.where(
                part == slot_row - float(cap * j), 1.0, 0.0
            ).astype(BF16)
        pos = dot(block, sel_pos)
        wts = dot(block, sel_w)
        weigh[pl.ds(j * rows, rows), :] = jnp.where(pos == r_col - float(cap * j), wts, 0.0).astype(BF16)

    def slot_rows(k, cc):
        return pl.ds(k * 2 * slab + mult(cc * slab, slab), slab)

    def dispatch(h, k, cc):
        return remote(
            slots.at[slot_rows(k, cc), cols(h)],
            recv.at[slot_rows(k, c), cols(h)],
            d_s.at[h, k * 2 + cc],
            d_r.at[h, k * 2 + c],
            ring2(k, cc),
        )

    def dispatch_in(h, k, cs):
        return remote(
            slots.at[slot_rows(k, cs), cols(h)],
            recv.at[slot_rows(k, cs), cols(h)],
            d_s.at[h, k * 2 + cs],
            d_r.at[h, k * 2 + cs],
            source(k, cs) if k else at(y, z, 1 - c),
        )

    def send_slots(h):
        for k in (2, 1, 3, 0):
            both = pl.ds(k * 2 * slab, 2 * slab)
            slots[both, cols(h)] = dot(place[both, :], ag[:, cols(h)]).astype(BF16)
            if k:
                for cc in range(2):
                    dispatch(h, k, cc).start()
            else:
                dispatch(h, 0, 1 - c).start()
                recv[slot_rows(0, c), cols(h)] = slots[slot_rows(0, c), cols(h)]

    def await_slots(h, k):
        if k:
            for cs in range(2):
                dispatch_in(h, k, cs).wait_recv()
        else:
            dispatch_in(h, 0, 1 - c).wait_recv()

    for j in (2, 1, 3):
        gather(0, j).wait_recv()
    send_slots(0)

    for t in range(2):
        dp_rows_in(t).wait_recv()

    def write_other(h, v):
        soth[h] = v.astype(BF16)

    shared(lambda h: x_in[h, :, pl.ds(0, half)], x_in[0, :, pl.ds(half, 128)][:, :1].astype(F32), write_other)

    def shared_back(t):
        return remote(soth.at[t], sh_in.at[tp], sh_s.at[t], sh_r.at[tp], (dpo, me, t))

    def shared_in(t):
        return remote(soth.at[t], sh_in.at[t], sh_s.at[t], sh_r.at[t], (dpo, me, t))

    for t in range(2):
        shared_back(t).start()

    for cp in loads[3:]:
        cp.wait()

    def first_half(k):
        await_slots(0, k)
        both = pl.ds(k * 2 * slab, 2 * slab)
        gacc[both, :] = dot(recv[both, cols(0)], gate[cols(0), :])
        uacc[both, :] = dot(recv[both, cols(0)], up[cols(0), :])

    first_half(0)
    for j in (2, 1, 3):
        gather(1, j).wait_recv()
    send_slots(1)
    for k in (1, 3, 2):
        first_half(k)

    def ret(f, fcols, k, cs):
        return remote(
            yout.at[slot_rows(k, cs), fcols],
            back.at[slot_rows(k, c), fcols],
            b_s.at[f, k * 2 + cs],
            b_r.at[f, k * 2 + c],
            source(k, cs) if k else at(y, z, 1 - c),
        )

    def ret_in(f, fcols, k, cc):
        return remote(
            yout.at[slot_rows(k, cc), fcols],
            back.at[slot_rows(k, cc), fcols],
            b_s.at[f, k * 2 + cc],
            b_r.at[f, k * 2 + cc],
            ring2(k, cc),
        )

    def project(f, fcols, k):
        both = pl.ds(k * 2 * slab, 2 * slab)
        yout[both, fcols] = dot(hid[both, :], down[:, fcols]).astype(BF16)
        if k:
            for cs in range(2):
                ret(f, fcols, k, cs).start()
        else:
            ret(f, fcols, 0, 1 - c).start()
            back[slot_rows(0, c), fcols] = yout[slot_rows(0, c), fcols]

    for k in ORDER:
        await_slots(1, k)
        both = pl.ds(k * 2 * slab, 2 * slab)
        g = gacc[both, :] + dot(recv[both, cols(1)], gate[cols(1), :])
        u = uacc[both, :] + dot(recv[both, cols(1)], up[cols(1), :])
        hid[both, :] = (silu(g) * u).astype(BF16)
        project(0, theirs, k)
    for k in ORDER:
        project(1, mine, k)

    def reduce(f, j):
        return remote(rs_out.at[f, j], rs_in.at[f, j], r_s.at[f, j], r_r.at[f, j], ring1((RING - j) % RING))

    def transfer():
        return remote(xfer_out, xfer_in, t_s, t_r, (dp, me, tpo))

    for f, fcols in ((0, theirs), (1, mine)):
        for k in ORDER:
            for cc in range(2) if k else (1 - c,):
                ret_in(f, fcols, k, cc).wait_recv()
        for j in (2, 1, 3):
            rs_out[f, j] = dot(weigh[pl.ds(j * rows, rows), :], back[:, fcols]).astype(BF16)
            reduce(f, j).start()
        own[f] = dot(weigh[pl.ds(0, rows), :], back[:, fcols]) + sown[:, fcols]

    def total(f):
        for j in (1, 3, 2):
            reduce(f, j).wait_recv()
        return own[f] + rs_in[f, 1].astype(F32) + rs_in[f, 3].astype(F32) + rs_in[f, 2].astype(F32)

    xfer_out[...] = total(0).astype(BF16)
    transfer().start()
    for t in range(2):
        shared_in(t).wait_recv()
    own[1] = total(1) + sh_in[0].astype(F32) + sh_in[1].astype(F32)
    transfer().wait_recv()
    out[...] = (own[1] + xfer_in[...].astype(F32)).astype(BF16)

    for h in range(2):
        for j in (2, 1, 3):
            gather(h, j).wait_send()
            reduce(h, j).wait_send()
        for k in range(1, RING):
            for cc in range(2):
                dispatch(h, k, cc).wait_send()
                ret(h, theirs, k, cc).wait_send()
        dispatch(h, 0, 1 - c).wait_send()
        ret(h, theirs, 0, 1 - c).wait_send()
        dp_rows(h).wait_send()
        shared_back(h).wait_send()
    for j in (2, 1, 3):
        meta_copy(j).wait_send()
    transfer().wait_send()


def per_device(
    tokens, norm_gain, router, expert_ids, modality, expert_gate, expert_up, expert_down, shared_gate, shared_up, shared_down
):
    rows, width = tokens.shape
    half = width // 2
    cap = 20
    hidden = expert_gate.shape[2]
    slot_count = 32 * cap
    dma = pltpu.SemaphoreType.DMA
    vm = pltpu.VMEM
    return pl.pallas_call(
        kernel,
        out_shape=jax.ShapeDtypeStruct((rows, half), BF16),
        in_specs=[pl.BlockSpec(memory_space=pltpu.VMEM)] * 5 + [pl.BlockSpec(memory_space=pl.ANY)] * 6,
        out_specs=pl.BlockSpec(memory_space=pltpu.VMEM),
        scratch_shapes=[
            vm(expert_gate.shape[1:], BF16),
            vm(expert_up.shape[1:], BF16),
            vm(expert_down.shape[1:], BF16),
            vm(shared_gate.shape, BF16),
            vm(shared_up.shape, BF16),
            vm(shared_down.shape, BF16),
            vm((RING * rows, width), BF16),
            vm((RING * rows, 128), BF16),
            vm((slot_count, 128), BF16),
            vm((slot_count, RING * rows), BF16),
            vm((RING * rows, slot_count), BF16),
            vm((slot_count, width), BF16),
            vm((slot_count, width), BF16),
            vm((slot_count, hidden), F32),
            vm((slot_count, hidden), F32),
            vm((slot_count, hidden), BF16),
            vm((slot_count, width), BF16),
            vm((slot_count, width), BF16),
            vm((2, RING, rows, half), BF16),
            vm((2, RING, rows, half), BF16),
            vm((rows, half + 128), BF16),
            vm((2, rows, half + 128), BF16),
            vm((rows, width), F32),
            vm((2, rows, half), BF16),
            vm((2, rows, half), BF16),
            vm((rows, half), BF16),
            vm((rows, half), BF16),
            vm((2, rows, half), F32),
            dma((6,)),
            dma((2, RING)), dma((2, RING)),
            dma((RING,)), dma((RING,)),
            dma((2,)), dma((2,)),
            dma((2, 8)), dma((2, 8)),
            dma((2, 8)), dma((2, 8)),
            dma((2, RING)), dma((2, RING)),
            dma((2,)), dma((2,)),
            dma, dma,
        ],
        compiler_params=pltpu.CompilerParams(
            collective_id=0, has_side_effects=True, vmem_limit_bytes=60 * 1024 * 1024
        ),
        name="moe_layer",
    )(
        tokens, norm_gain.reshape(1, width), router, expert_ids, modality.reshape(1, rows),
        expert_gate, expert_up, expert_down, shared_gate, shared_up, shared_down,
    )


def solution(mesh):
    in_specs = (
        P(("dp", "expert"), None),
        P(),
        P(),
        P(("dp", "expert"), None),
        P(("dp", "expert")),
        P("expert", None, "tensor"),
        P("expert", None, "tensor"),
        P("expert", "tensor", None),
        P(None, None, ("dp", "tensor")),
        P(None, None, ("dp", "tensor")),
        P(None, ("dp", "tensor"), None),
    )
    out_specs = P(("dp", "expert"), "tensor")
    return jax.shard_map(per_device, mesh=mesh, in_specs=in_specs, out_specs=out_specs, check_vma=False)
```

```python
import jax
import jax.numpy as jnp
from jax import lax
from jax.experimental import pallas as pl
from jax.experimental.pallas import tpu as pltpu
from jax.sharding import PartitionSpec as P

MESH = pl.DeviceIdType.MESH
F32, BF16 = jnp.float32, jnp.bfloat16
RING = 4
EPS = 1e-06
UNPICKED = -100.0
ORDER = (0, 1, 3, 2)


def dot(a, b):
    return lax.dot_general(a, b, (((1,), (0,)), ((), ())), preferred_element_type=F32)


def dot_t(a, b):
    return lax.dot_general(a, b, (((1,), (1,)), ((), ())), preferred_element_type=F32)


def silu(v):
    return v / (1.0 + jnp.exp(-v))


def kernel(
    tokens, gain, router, ids, flags, gate_h, up_h, down_h, sgate_h, sup_h, sdown_h, out,
    gate, up, down, sgate, sup, sdown,
    ag, meta, sel, place, weigh, slots, recv, gacc, uacc, hid, yout, back, rs_out, rs_in,
    x_out, x_in, sown, soth, sh_in, xfer_out, xfer_in, own,
    w_sem, g_s, g_r, m_s, m_r, xs_s, xs_r, d_s, d_r, b_s, b_r, r_s, r_r, sh_s, sh_r, t_s, t_r,
):
    rows, width = tokens.shape
    half = width // 2
    cap = recv.shape[0] // 32
    slab = RING * cap
    dp, me, tp = lax.axis_index("dp"), lax.axis_index("expert"), lax.axis_index("tensor")
    y, z, c = me // 8, (me % 8) // 2, me % 2
    dpo, tpo = 1 - dp, 1 - tp

    def at(yy, zz, cc):
        return (dp, yy * 8 + zz * 2 + cc, tp)

    def along_y(k):
        return (y + k) % RING

    def along_z(k):
        return (z + k) % RING

    def ring1(k):
        return at(c * along_y(k) + (1 - c) * y, (1 - c) * along_z(k) + c * z, c)

    def expert_of(k, cc):
        return (c * y + (1 - c) * along_y(k)) * 8 + (c * along_z(k) + (1 - c) * z) * 2 + cc

    def ring2(k, cc):
        return (dp, expert_of(k, cc), tp)

    def source(k, cs):
        return at(along_y(RING - k), z, 0) if cs == 0 else at(y, along_z(RING - k), 1)

    def mult(v, m):
        return pl.multiple_of(v, m)

    loads = [
        pltpu.make_async_copy(s, d, w_sem.at[i])
        for i, (s, d) in enumerate(
            [(sgate_h, sgate), (sup_h, sup), (sdown_h, sdown), (gate_h.at[0], gate), (up_h.at[0], up), (down_h.at[0], down)]
        )
    ]
    for cp in loads:
        cp.start()

    barrier = pltpu.get_barrier_semaphore()
    peers = [at(y, z, 1 - c), (dpo, me, 0), (dpo, me, 1), (dp, me, tpo)]
    for k in range(1, RING):
        for cc in range(2):
            peers += [at(along_y(k), z, cc), at(y, along_z(k), cc)]
    for peer in peers:
        pl.semaphore_signal(barrier, inc=1, device_id=peer, device_id_type=MESH)

    def remote(src, dst, ssem, rsem, dev):
        return pltpu.make_async_remote_copy(
            src_ref=src, dst_ref=dst, send_sem=ssem, recv_sem=rsem, device_id=dev, device_id_type=MESH
        )

    step = 32

    def norm_rows(i, carry):
        at_rows = pl.ds(mult(i * step, step), step)
        v = tokens[at_rows, :].astype(F32)
        inv = lax.rsqrt(jnp.mean(v * v, axis=-1, keepdims=True) + EPS)
        ag[at_rows, :] = (v * inv * gain[...]).astype(BF16)
        return carry

    lax.fori_loop(0, rows // step, norm_rows, 0)
    pl.semaphore_wait(barrier, len(peers))

    def cols(h):
        return pl.ds(h * half, half)

    def gather(h, j):
        return remote(
            ag.at[pl.ds(0, rows), cols(h)], ag.at[pl.ds(j * rows, rows), cols(h)], g_s.at[h, j], g_r.at[h, j], ring1(j)
        )

    for j in (2, 1, 3):
        gather(0, j).start()

    mine = pl.ds(mult(tp * half, half), half)
    theirs = pl.ds(mult(tpo * half, half), half)
    flag_rows = jnp.transpose(jnp.broadcast_to(flags[...].astype(F32), (rows, rows)))
    x_out[:, pl.ds(0, half)] = ag[pl.ds(0, rows), mine]
    x_out[:, pl.ds(half, 128)] = flag_rows.astype(BF16)

    def dp_rows(t):
        return remote(x_out, x_in.at[tp], xs_s.at[t], xs_r.at[tp], (dpo, me, t))

    def dp_rows_in(t):
        return remote(x_out, x_in.at[t], xs_s.at[t], xs_r.at[t], (dpo, me, t))

    for t in range(2):
        dp_rows(t).start()

    lane = lax.broadcasted_iota(jnp.int32, (rows, rows), 1)
    sub = lax.broadcasted_iota(jnp.int32, (rows, rows), 0)
    expert_row = lax.broadcasted_iota(jnp.int32, (32, rows), 0)
    chosen = jnp.zeros((32, rows), F32)
    for k in range(ids.shape[0]):
        chosen = chosen + (ids[k : k + 1, :] == expert_row).astype(F32)
    earlier = (sub < lane).astype(BF16)
    rank = dot(chosen.astype(BF16), earlier)
    logits = dot_t(router[...], ag[pl.ds(0, rows), :])
    score = chosen / (1.0 + jnp.exp(-logits))
    meta[pl.ds(0, 32), :] = jnp.where(chosen > 0.0, rank, UNPICKED).astype(BF16)
    meta[pl.ds(32, 32), :] = (score / jnp.sum(score, axis=0, keepdims=True)).astype(BF16)

    def meta_copy(j):
        return remote(meta.at[pl.ds(0, 64)], meta.at[pl.ds(j * 64, 64)], m_s.at[j], m_r.at[j], ring1(j))

    for j in (2, 1, 3):
        meta_copy(j).start()
    for j in (2, 1, 3):
        gather(1, j).start()

    for cp in loads[:3]:
        cp.wait()

    def shared(read_rows, keep, write):
        hidden = []
        for m in range(2):
            g = jnp.zeros((rows, sgate.shape[1]), F32)
            u = jnp.zeros((rows, sgate.shape[1]), F32)
            for h in range(2):
                part = read_rows(h)
                g = g + dot_t(part, sgate[m, :, cols(h)])
                u = u + dot_t(part, sup[m, :, cols(h)])
            picked = keep if m == 0 else 1.0 - keep
            hidden.append((silu(g) * u * picked).astype(BF16))
        for h in range(2):
            write(h, dot(hidden[0], sdown[0, :, cols(h)]) + dot(hidden[1], sdown[1, :, cols(h)]))

    def write_own(h, v):
        sown[:, cols(h)] = v

    shared(lambda h: ag[pl.ds(0, rows), cols(h)], flag_rows[:, :1], write_own)

    for s in range(8):
        e = expert_of(s // 2, s % 2)
        sel[pl.ds(s * slab, slab), :] = (lax.broadcasted_iota(jnp.int32, (slab, 64), 1) == e).astype(BF16)
    for j in (2, 1, 3):
        meta_copy(j).wait_recv()
    slot_row = lax.broadcasted_iota(jnp.int32, (slab, rows), 0).astype(F32)
    col = lax.broadcasted_iota(jnp.int32, (1, 8 * slab), 1)
    e_col = jnp.zeros((1, 8 * slab), jnp.int32)
    r_col = col
    for s in range(8):
        inside = (col >= s * slab) & (col < (s + 1) * slab)
        e_col = jnp.where(inside, expert_of(s // 2, s % 2), e_col)
        r_col = jnp.where(inside, col - s * slab, r_col)
    r_col = r_col.astype(F32)
    wide = lax.broadcasted_iota(jnp.int32, (128, 8 * slab), 0)
    sel_pos = (wide == e_col).astype(BF16)
    sel_w = (wide == e_col + 32).astype(BF16)
    for j in range(RING):
        turned = meta[pl.ds(j * 64, 64), :]
        block = jnp.transpose(jnp.concatenate([turned.astype(F32)] * 2, axis=0)).astype(BF16)
        turned_pos = dot(sel[...], turned)
        for s in range(8):
            part = turned_pos[s * slab : (s + 1) * slab, :]
            place[pl.ds(s * slab, slab), pl.ds(j * rows, rows)] = jnp.where(
                part == slot_row - float(cap * j), 1.0, 0.0
            ).astype(BF16)
        pos = dot(block, sel_pos)
        wts = dot(block, sel_w)
        weigh[pl.ds(j * rows, rows), :] = jnp.where(pos == r_col - float(cap * j), wts, 0.0).astype(BF16)

    def slot_rows(k, cc):
        return pl.ds(k * 2 * slab + mult(cc * slab, slab), slab)

    def dispatch(h, k, cc):
        return remote(
            slots.at[slot_rows(k, cc), cols(h)],
            recv.at[slot_rows(k, c), cols(h)],
            d_s.at[h, k * 2 + cc],
            d_r.at[h, k * 2 + c],
            ring2(k, cc),
        )

    def dispatch_in(h, k, cs):
        return remote(
            slots.at[slot_rows(k, cs), cols(h)],
            recv.at[slot_rows(k, cs), cols(h)],
            d_s.at[h, k * 2 + cs],
            d_r.at[h, k * 2 + cs],
            source(k, cs) if k else at(y, z, 1 - c),
        )

    def send_slots(h):
        for k in (2, 1, 3, 0):
            both = pl.ds(k * 2 * slab, 2 * slab)
            slots[both, cols(h)] = dot(place[both, :], ag[:, cols(h)]).astype(BF16)
            if k:
                for cc in range(2):
                    dispatch(h, k, cc).start()
            else:
                dispatch(h, 0, 1 - c).start()
                recv[slot_rows(0, c), cols(h)] = slots[slot_rows(0, c), cols(h)]

    def await_slots(h, k):
        if k:
            for cs in range(2):
                dispatch_in(h, k, cs).wait_recv()
        else:
            dispatch_in(h, 0, 1 - c).wait_recv()

    for j in (2, 1, 3):
        gather(0, j).wait_recv()
    send_slots(0)

    for t in range(2):
        dp_rows_in(t).wait_recv()

    def write_other(h, v):
        soth[h] = v.astype(BF16)

    shared(lambda h: x_in[h, :, pl.ds(0, half)], x_in[0, :, pl.ds(half, 128)][:, :1].astype(F32), write_other)

    def shared_back(t):
        return remote(soth.at[t], sh_in.at[tp], sh_s.at[t], sh_r.at[tp], (dpo, me, t))

    def shared_in(t):
        return remote(soth.at[t], sh_in.at[t], sh_s.at[t], sh_r.at[t], (dpo, me, t))

    for t in range(2):
        shared_back(t).start()

    for cp in loads[3:]:
        cp.wait()

    def first_half(k):
        await_slots(0, k)
        both = pl.ds(k * 2 * slab, 2 * slab)
        gacc[both, :] = dot_t(recv[both, cols(0)], gate[:, cols(0)])
        uacc[both, :] = dot_t(recv[both, cols(0)], up[:, cols(0)])

    first_half(0)
    for j in (2, 1, 3):
        gather(1, j).wait_recv()
    send_slots(1)
    for k in (1, 3, 2):
        first_half(k)

    def ret(f, fcols, k, cs):
        return remote(
            yout.at[slot_rows(k, cs), fcols],
            back.at[slot_rows(k, c), fcols],
            b_s.at[f, k * 2 + cs],
            b_r.at[f, k * 2 + c],
            source(k, cs) if k else at(y, z, 1 - c),
        )

    def ret_in(f, fcols, k, cc):
        return remote(
            yout.at[slot_rows(k, cc), fcols],
            back.at[slot_rows(k, cc), fcols],
            b_s.at[f, k * 2 + cc],
            b_r.at[f, k * 2 + cc],
            ring2(k, cc),
        )

    def project(f, fcols, k):
        both = pl.ds(k * 2 * slab, 2 * slab)
        yout[both, fcols] = dot(hid[both, :], down[:, fcols]).astype(BF16)
        if k:
            for cs in range(2):
                ret(f, fcols, k, cs).start()
        else:
            ret(f, fcols, 0, 1 - c).start()
            back[slot_rows(0, c), fcols] = yout[slot_rows(0, c), fcols]

    for k in ORDER:
        await_slots(1, k)
        both = pl.ds(k * 2 * slab, 2 * slab)
        g = gacc[both, :] + dot_t(recv[both, cols(1)], gate[:, cols(1)])
        u = uacc[both, :] + dot_t(recv[both, cols(1)], up[:, cols(1)])
        hid[both, :] = (silu(g) * u).astype(BF16)
        project(0, theirs, k)
    for k in ORDER:
        project(1, mine, k)

    def reduce(f, j):
        return remote(rs_out.at[f, j], rs_in.at[f, j], r_s.at[f, j], r_r.at[f, j], ring1((RING - j) % RING))

    def transfer():
        return remote(xfer_out, xfer_in, t_s, t_r, (dp, me, tpo))

    for f, fcols in ((0, theirs), (1, mine)):
        for k in ORDER:
            for cc in range(2) if k else (1 - c,):
                ret_in(f, fcols, k, cc).wait_recv()
        for j in (2, 1, 3):
            rs_out[f, j] = dot(weigh[pl.ds(j * rows, rows), :], back[:, fcols]).astype(BF16)
            reduce(f, j).start()
        own[f] = dot(weigh[pl.ds(0, rows), :], back[:, fcols]) + sown[:, fcols]

    def total(f):
        for j in (1, 3, 2):
            reduce(f, j).wait_recv()
        return own[f] + rs_in[f, 1].astype(F32) + rs_in[f, 3].astype(F32) + rs_in[f, 2].astype(F32)

    xfer_out[...] = total(0).astype(BF16)
    transfer().start()
    for t in range(2):
        shared_in(t).wait_recv()
    own[1] = total(1) + sh_in[0].astype(F32) + sh_in[1].astype(F32)
    transfer().wait_recv()
    out[...] = (own[1] + xfer_in[...].astype(F32)).astype(BF16)

    for h in range(2):
        for j in (2, 1, 3):
            gather(h, j).wait_send()
            reduce(h, j).wait_send()
        for k in range(1, RING):
            for cc in range(2):
                dispatch(h, k, cc).wait_send()
                ret(h, theirs, k, cc).wait_send()
        dispatch(h, 0, 1 - c).wait_send()
        ret(h, theirs, 0, 1 - c).wait_send()
        dp_rows(h).wait_send()
        shared_back(h).wait_send()
    for j in (2, 1, 3):
        meta_copy(j).wait_send()
    transfer().wait_send()


def per_device(
    tokens, norm_gain, router, expert_ids, modality, expert_gate, expert_up, expert_down, shared_gate, shared_up, shared_down
):
    rows, width = tokens.shape
    half = width // 2
    cap = 20
    hidden = expert_gate.shape[2]
    part = shared_gate.shape[2]
    slot_count = 32 * cap
    dma = pltpu.SemaphoreType.DMA
    vm = pltpu.VMEM
    return pl.pallas_call(
        kernel,
        out_shape=jax.ShapeDtypeStruct((rows, half), BF16),
        in_specs=[pl.BlockSpec(memory_space=pltpu.VMEM)] * 5 + [pl.BlockSpec(memory_space=pl.ANY)] * 6,
        out_specs=pl.BlockSpec(memory_space=pltpu.VMEM),
        scratch_shapes=[
            vm((hidden, width), BF16),
            vm((hidden, width), BF16),
            vm((hidden, width), BF16),
            vm((2, part, width), BF16),
            vm((2, part, width), BF16),
            vm(shared_down.shape, BF16),
            vm((RING * rows, width), BF16),
            vm((RING * 64, rows), BF16),
            vm((slot_count, 64), BF16),
            vm((slot_count, RING * rows), BF16),
            vm((RING * rows, slot_count), BF16),
            vm((slot_count, width), BF16),
            vm((slot_count, width), BF16),
            vm((slot_count, hidden), F32),
            vm((slot_count, hidden), F32),
            vm((slot_count, hidden), BF16),
            vm((slot_count, width), BF16),
            vm((slot_count, width), BF16),
            vm((2, RING, rows, half), BF16),
            vm((2, RING, rows, half), BF16),
            vm((rows, half + 128), BF16),
            vm((2, rows, half + 128), BF16),
            vm((rows, width), F32),
            vm((2, rows, half), BF16),
            vm((2, rows, half), BF16),
            vm((rows, half), BF16),
            vm((rows, half), BF16),
            vm((2, rows, half), F32),
            dma((6,)),
            dma((2, RING)), dma((2, RING)),
            dma((RING,)), dma((RING,)),
            dma((2,)), dma((2,)),
            dma((2, 8)), dma((2, 8)),
            dma((2, 8)), dma((2, 8)),
            dma((2, RING)), dma((2, RING)),
            dma((2,)), dma((2,)),
            dma, dma,
        ],
        compiler_params=pltpu.CompilerParams(
            collective_id=0, has_side_effects=True, vmem_limit_bytes=60 * 1024 * 1024
        ),
        name="moe_layer",
    )(
        tokens, norm_gain.reshape(1, width), router.T, expert_ids.T, modality.reshape(1, rows),
        expert_gate.swapaxes(1, 2), expert_up.swapaxes(1, 2), expert_down,
        shared_gate.swapaxes(1, 2), shared_up.swapaxes(1, 2), shared_down,
    )


def solution(mesh):
    in_specs = (
        P(("dp", "expert"), None),
        P(),
        P(),
        P(("dp", "expert"), None),
        P(("dp", "expert")),
        P("expert", None, "tensor"),
        P("expert", None, "tensor"),
        P("expert", "tensor", None),
        P(None, None, ("dp", "tensor")),
        P(None, None, ("dp", "tensor")),
        P(None, ("dp", "tensor"), None),
    )
    out_specs = P(("dp", "expert"), "tensor")
    return jax.shard_map(per_device, mesh=mesh, in_specs=in_specs, out_specs=out_specs, check_vma=False)
```
